32 devices in a mesh: band: 4 (over y, x), fft: 8 (over z, core).
Axes of the slice: x: 2, y: 2, z: 4, core: 2. Of those that a mesh axis runs over, the one named last changes fastest.
Arguments:
- wave: float32 [2, 8, 128, 128, 128], P(None, 'band', 'fft'), may hold values from -6 to 6
- previous: float32 [2, 8, 128, 128, 128], P(None, 'band', 'fft'), may hold values from -6 to 6
- potential: float32 [128, 128, 128], P('band', 'fft'), may hold values from -1.5 to 1.5
- column_extent: int32 [128, 128], P('fft'), may hold values from -1 to 31, as said below
- metric: float32 [3], replicated, may hold values from 0.5 to 2
- center: float32 [1], replicated, may hold values from 0.5 to 2
- halfwidth: float32 [1], replicated, may hold values from 1 to 3
Outputs:
- filtered: float32 [2, 8, 128, 128, 128], P(None, 'band', 'fft')
The draws below stay inside these ranges and needn't reach their ends.
Inputs may be any that keep to these rules, and one draw needn't show every extreme that they name: `column_extent`: every entry is -1 where |s(gx)| >= 32 or |s(gy)| >= 32, with s the signed index of the steps. Some column reaches the maximum.
All inputs are finite; a program needn't handle non-finite values.
Results may differ from the reference program's by a relative error of at most 0.00005.
Values sent between devices are 32-bit elements; how exact they have to be, the bound alone decides.
A program may use at most 64 MiB of HBM per device.

```python
import math
import jax
import jax.numpy as jnp
from jax import lax

NX = 128
NY = 128
NZ = 128
BANDS = 8


def draw_column_extent(key, part):
    first_key, second_key = jax.random.split(key, 2)
    weights = jax.random.randint(first_key, (3,), 1, 5).astype(jnp.int32)
    largest = NZ // 4 - 1
    base_room = weights[2] * largest * largest
    radius_sq = base_room + jax.random.randint(second_key, (), 0, 1024).astype(jnp.int32) * (base_room // 1024 + 1)
    index_x = jnp.arange(NX, dtype=jnp.int32)
    index_y = jnp.arange(NY, dtype=jnp.int32)
    signed_x = jnp.where(index_x < NX // 2, index_x, index_x - NX)
    signed_y = jnp.where(index_y < NY // 2, index_y, index_y - NY)
    room_left = radius_sq - weights[0] * signed_x[:, None] ** 2 - weights[1] * signed_y[None, :] ** 2
    heights = jnp.arange(largest + 1, dtype=jnp.int32)
    counted = jnp.sum((weights[2] * heights[None, None, :] ** 2 <= room_left[:, :, None]).astype(jnp.int32), axis=2) - 1
    in_box = (jnp.abs(signed_x)[:, None] < NX // 4) & (jnp.abs(signed_y)[None, :] < NY // 4)
    return jnp.where(in_box, counted, -1).astype(jnp.int32)


def shard_levels(key, dims, shards, smallest, high):
    factor_of, own = 1.0, jax.random.fold_in(key, 6)
    for dim, blocks in shards:
        steps = jnp.exp(jax.random.uniform(jax.random.fold_in(own, dim), (blocks,), jnp.float32, smallest / len(shards), high / len(shards)))
        factor_of = factor_of * jnp.repeat(steps, dims[dim] // blocks).reshape([-1 if axis == dim else 1 for axis in range(len(dims))])
    return factor_of


def noise(rng, extent, deviation, bound, cuts=(), kind=jnp.bfloat16):
    values = jax.random.normal(rng, extent, jnp.float32) * deviation
    if len(cuts) > 0:
        values = shard_levels(rng, extent, cuts, -0.22, 0.18) * values
    return jnp.clip(values, min=-bound, max=bound).astype(kind)


def setup_inputs(seed: int = 0) -> dict:
    keys = jax.random.split(jax.random.key(seed), 8)
    return {
        "wave": noise(keys[0], (2, BANDS, NX, NZ, NY), 1.0, 6.0, ((1, 4), (2, 8)), jnp.float32),
        "previous": noise(keys[1], (2, BANDS, NX, NZ, NY), 1.0, 6.0, ((1, 4), (2, 8)), jnp.float32),
        "potential": jnp.clip(jax.random.uniform(keys[2], (NX, NZ, NY), jnp.float32, -1.5, 1.5) * shard_levels(keys[2], (NX, NZ, NY), ((0, 4), (1, 8)), -0.4, 0.0), -1.5, 1.5),
        "column_extent": draw_column_extent(jax.random.fold_in(keys[7], 71), 0),
        "metric": jnp.clip(jnp.exp(jax.random.uniform(keys[4], (3,), jnp.float32, math.log(0.5), math.log(2.0))), 0.5, 2.0),
        "center": jnp.clip(jax.random.uniform(keys[5], (1,), jnp.float32, 0.5, 2.0), 0.5, 2.0),
        "halfwidth": jnp.clip(jnp.exp(jax.random.uniform(keys[6], (1,), jnp.float32, math.log(1.0), math.log(3.0))), 1.0, 3.0),
    }


def signed(length):
    indices = jnp.arange(length, dtype=jnp.int32)
    return jnp.where(indices < length // 2, indices, indices - length)


def reference(wave, previous, potential, column_extent, metric, center, halfwidth):
    keep_mask = (jnp.abs(signed(NZ))[None, :, None] <= column_extent[:, None, :]).astype(jnp.float32)
    two_pi = 2.0 * math.pi
    kinetic_x = (two_pi * signed(NX).astype(jnp.float32) / NX) ** 2
    kinetic_y = (two_pi * signed(NY).astype(jnp.float32) / NY) ** 2
    kinetic_z = (two_pi * signed(NZ).astype(jnp.float32) / NZ) ** 2
    kinetic = 0.5 * (metric[0] * kinetic_x[:, None, None] + metric[2] * kinetic_z[None, :, None] + metric[1] * kinetic_y[None, None, :])
    cell_count = NX * NY * NZ
    factor = 2.0 / halfwidth[0]

    def one_band(pieces):
        real_in, imag_in, real_prev, imag_prev = pieces
        coefficient = (real_in + 1j * imag_in) * keep_mask
        real_space = jnp.fft.ifftn(coefficient) * cell_count
        potential_term = jnp.fft.fftn(potential * real_space) / cell_count
        applied = kinetic * coefficient + potential_term
        result = keep_mask * (factor * (applied - center[0] * coefficient) - (real_prev + 1j * imag_prev))
        return jnp.real(result).astype(jnp.float32), jnp.imag(result).astype(jnp.float32)

    real_out, imag_out = lax.map(one_band, (wave[0], wave[1], previous[0], previous[1]))
    return jnp.stack([real_out, imag_out])
```

```python
import math

import jax
import jax.numpy as jnp
import functools
import numpy as np
from jax import lax
from jax.experimental import pallas as pl
from jax.experimental.pallas import tpu as pltpu
from jax.sharding import PartitionSpec as P

NX = 128
NY = 128
NZ = 128


def signed(length):
    indices = jnp.arange(length, dtype=jnp.int32)
    return jnp.where(indices < length // 2, indices, indices - length)


def tables(length, forward):
    indices = jnp.arange(length, dtype=jnp.int32)
    phases = indices[:, None] * indices[None, :] % length
    angles = phases.astype(jnp.float32) * (2.0 * math.pi / length)
    cosine_table = jnp.cos(angles)
    sine_table = jnp.sin(angles)
    if forward:
        return (cosine_table / length, -sine_table / length)
    return (cosine_table, sine_table)


def transform(real_part, imag_part, cosine_table, sine_table, form):
    highest = lax.Precision.HIGHEST
    real_cos = jnp.einsum(form, real_part, cosine_table, precision=highest)
    imag_sin = jnp.einsum(form, imag_part, sine_table, precision=highest)
    real_sin = jnp.einsum(form, real_part, sine_table, precision=highest)
    imag_cos = jnp.einsum(form, imag_part, cosine_table, precision=highest)
    return (real_cos - imag_sin, real_sin + imag_cos)


def local(wave, previous, potential, column_extent, metric, center, halfwidth):
    gx_local = wave.shape[2]
    quarter = NY // 4
    keep_mask = (jnp.abs(signed(NZ))[None, :, None] <= column_extent[:, None, :]).astype(
        jnp.float32
    )
    coeff_real = wave[0] * keep_mask
    coeff_imag = wave[1] * keep_mask
    inverse_z = tables(NZ, False)
    real_part, imag_part = transform(
        coeff_real, coeff_imag, inverse_z[0], inverse_z[1], "bxgy,gz->bxzy"
    )
    full_potential = lax.all_gather(potential, "band", axis=0, tiled=True)
    inverse_x = tables(NX, False)
    forward_x = tables(NX, True)
    inverse_y = tables(NY, False)
    forward_y = tables(NY, True)
    forward_z = tables(NZ, True)
    real_part = jnp.concatenate([real_part[..., :quarter], real_part[..., NY - quarter :]], axis=-1)
    imag_part = jnp.concatenate([imag_part[..., :quarter], imag_part[..., NY - quarter :]], axis=-1)
    inverse_y = tuple(
        (jnp.concatenate([table[:quarter], table[NY - quarter :]], axis=0) for table in inverse_y)
    )
    forward_y = tuple(
        (
            jnp.concatenate([table[:, :quarter], table[:, NY - quarter :]], axis=1)
            for table in forward_y
        )
    )
    real_in = lax.all_to_all(real_part, "fft", split_axis=2, concat_axis=1, tiled=True)
    imag_in = lax.all_to_all(imag_part, "fft", split_axis=2, concat_axis=1, tiled=True)
    real_in, imag_in = transform(real_in, imag_in, inverse_y[0], inverse_y[1], "bxzg,gy->bxzy")
    real_in, imag_in = transform(real_in, imag_in, inverse_x[0], inverse_x[1], "bgzy,gx->bxzy")
    real_in = real_in * full_potential
    imag_in = imag_in * full_potential
    real_in, imag_in = transform(real_in, imag_in, forward_x[0], forward_x[1], "bxzy,xg->bgzy")
    real_part, imag_part = transform(real_in, imag_in, forward_y[0], forward_y[1], "bgzy,yk->bgzk")
    real_part, imag_part = transform(
        lax.all_to_all(real_part, "fft", split_axis=1, concat_axis=2, tiled=True),
        lax.all_to_all(imag_part, "fft", split_axis=1, concat_axis=2, tiled=True),
        forward_z[0],
        forward_z[1],
        "bxzy,zg->bxgy",
    )
    padding = jnp.zeros(real_part.shape[:-1] + (NY - 2 * quarter,), jnp.float32)
    real_part = jnp.concatenate(
        [real_part[..., :quarter], padding, real_part[..., quarter:]], axis=-1
    )
    imag_part = jnp.concatenate(
        [imag_part[..., :quarter], padding, imag_part[..., quarter:]], axis=-1
    )
    global_x = lax.axis_index("fft") * gx_local + jnp.arange(gx_local, dtype=jnp.int32)
    signed_x = jnp.where(global_x < NX // 2, global_x, global_x - NX)
    two_pi = 2.0 * math.pi
    kinetic_x = (two_pi * signed_x.astype(jnp.float32) / NX) ** 2
    kinetic_y = (two_pi * signed(NY).astype(jnp.float32) / NY) ** 2
    kinetic_z = (two_pi * signed(NZ).astype(jnp.float32) / NZ) ** 2
    kinetic = 0.5 * (
        metric[0] * kinetic_x[:, None, None]
        + metric[2] * kinetic_z[None, :, None]
        + metric[1] * kinetic_y[None, None, :]
    )
    factor = 2.0 / halfwidth[0]
    out_real = keep_mask * (
        factor * (kinetic * coeff_real + real_part - center[0] * coeff_real) - previous[0]
    )
    out_imag = keep_mask * (
        factor * (kinetic * coeff_imag + imag_part - center[0] * coeff_imag) - previous[1]
    )
    return jnp.stack([out_real, out_imag])


def roots(rows, columns, length):
    phases = np.outer(rows, columns) % length
    angles = phases * (2.0 * np.pi / length)
    return np.cos(angles), np.sin(angles)


def halves(table):
    table = jnp.asarray(table.astype(np.float32))
    high = table.astype(jnp.bfloat16)
    low = (table - high.astype(jnp.float32)).astype(jnp.bfloat16)
    return jnp.stack([high, low])


def boxed(length):
    return np.concatenate([np.arange(length // 4), np.arange(length - length // 4, length)])


def dft_tables():
    cos_z, sin_z = roots(np.arange(NZ), boxed(NZ), NZ)
    cos_x, sin_x = roots(np.arange(NX), boxed(NX), NX)
    lanes = np.arange(NY)
    is_real = (lanes < NY // 4) | (lanes >= NY - NY // 4)
    gy = np.where(is_real, lanes, (lanes + NY // 2) % NY)
    cos_y, sin_y = roots(gy, np.arange(NY), NY)
    real = is_real[:, None]
    inverse_y = np.concatenate([np.where(real, cos_y, -sin_y), np.where(real, sin_y, cos_y)], axis=1)
    forward_y = np.concatenate([np.where(real, cos_y, -sin_y).T, np.where(real, sin_y, cos_y).T]) / NY
    return (
        halves(np.concatenate([cos_z, sin_z], axis=1)),
        halves(inverse_y),
        halves(np.concatenate([cos_x, sin_x], axis=1)),
        halves(np.concatenate([cos_x.T, -sin_x.T], axis=1) / NX),
        halves(forward_y),
        halves(np.concatenate([cos_z.T, -sin_z.T], axis=1) / NZ),
    )


def split(value):
    high = value.astype(jnp.bfloat16)
    return high, (value - high.astype(jnp.float32)).astype(jnp.bfloat16)


def dot(a, b):
    return jnp.dot(a, b, preferred_element_type=jnp.float32)


def table_left(table, high, low):
    return dot(table[0], high) + (dot(table[0], low) + dot(table[1], high))


def table_right(value, table):
    high, low = split(value)
    return dot(high, table[0]) + (dot(low, table[0]) + dot(high, table[1]))


def times_i(value):
    half = value.shape[1] // 2
    return jnp.concatenate([-value[:, half:], value[:, :half]], axis=1)


def with_i(value):
    high, low = split(value)
    return (
        jnp.concatenate([high, times_i(high)], axis=0),
        jnp.concatenate([low, times_i(low)], axis=0),
    )


def packed_i(value):
    lane = lax.broadcasted_iota(jnp.int32, value.shape, 1)
    is_real = (lane < NY // 4) | (lane >= NY - NY // 4)
    turned = pltpu.roll(value, NY // 2, 1)
    return jnp.where(is_real, -turned, turned)


def exchange(
    groups, peers,
    metric, center, halfwidth, wave, previous, potential, extent, *rest,
):
    table_refs, (compact,), rest = rest[:6], rest[6:7], rest[7:]
    tables_in, rest = rest[:6], rest[6:]
    inv_z, inv_y, inv_x, fwd_x, fwd_y, fwd_z = tables_in
    waves, prevs, send1, recv1, vbuf, send2, recv2 = rest[:7]
    table_sem, wave_sem, prev_sem, vown_sem, own1_sem, own2_sem, *rest = rest[7:]
    vsend, vrecv, ssend1, srecv1, ssend2, srecv2 = rest
    bands, gxl = wave.shape[1], wave.shape[2]
    quarter = NZ // 4
    active = peers // 2
    zl = NZ // peers
    block = zl * gxl
    depth = 4 if zl % 4 == 0 else 1
    chunks = zl // depth
    piece = depth * gxl
    kept_x = active * gxl
    group = lax.axis_index("band")
    me = lax.axis_index("fft")
    is_active = (me < peers // 4) | (me >= peers - peers // 4)
    mine = jnp.where(me < peers // 4, me, me - peers // 2)
    vrows = potential.shape[0]

    def device_of(a):
        return jnp.where(a < active // 2, a, a + peers // 2)

    def load(source, target, sem, b, part, half):
        return pltpu.make_async_copy(
            source.at[part, b, :, pl.ds(half * (NZ - quarter), quarter), :],
            target.at[b, part, half],
            sem.at[b, part, half],
        )

    loads = [(b, part, half) for b in range(bands) for part in range(2) for half in range(2)]
    fetches = [
        pltpu.make_async_copy(table_refs[i], tables_in[i], table_sem.at[i]) for i in range(6)
    ]

    @pl.when(is_active)
    def _():
        for where in loads:
            load(wave, waves, wave_sem, *where).start()

    for fetch in fetches:
        fetch.start()

    vown = pltpu.make_async_copy(
        potential, vbuf.at[pl.ds(group * vrows, vrows), :], vown_sem.at[0]
    )
    vown.start()

    barrier = pltpu.get_barrier_semaphore()

    def greet_fft(k, c):
        pl.semaphore_signal(barrier, inc=1, device_id={"fft": (me + k) % peers})
        return c

    def greet_band(k, c):
        pl.semaphore_signal(barrier, inc=1, device_id={"band": (group + k) % groups})
        return c

    lax.fori_loop(1, peers, greet_fft, 0)
    lax.fori_loop(1, groups, greet_band, 0)
    pl.semaphore_wait(barrier, peers - 1 + groups - 1)

    def vcopy(k):
        return pltpu.make_async_remote_copy(
            src_ref=potential,
            dst_ref=vbuf.at[pl.ds(group * vrows, vrows), :],
            send_sem=vsend.at[k],
            recv_sem=vrecv.at[k],
            device_id={"band": (group + k) % groups},
        )

    def vstart(k, c):
        vcopy(k).start()
        return c

    def out1(b, c, d):
        return pltpu.make_async_remote_copy(
            src_ref=send1.at[b, pl.ds(d * block + c * piece, piece), :],
            dst_ref=recv1.at[b, mine, pl.ds(c * piece, piece), :],
            send_sem=ssend1.at[b, c, d],
            recv_sem=srecv1.at[b, c, mine],
            device_id={"fft": d},
        )

    def in1(b, c, a):
        return pltpu.make_async_remote_copy(
            src_ref=send1.at[b, pl.ds(0, piece), :],
            dst_ref=recv1.at[b, a, pl.ds(c * piece, piece), :],
            send_sem=ssend1.at[b, c, 0],
            recv_sem=srecv1.at[b, c, a],
            device_id={"fft": (me + 1) % peers},
        )

    def out2(b, c, a):
        return pltpu.make_async_remote_copy(
            src_ref=send2.at[b, a, pl.ds(c * piece, piece), :],
            dst_ref=recv2.at[b, pl.ds(me * block + c * piece, piece), :],
            send_sem=ssend2.at[b, c, a],
            recv_sem=srecv2.at[b, c, me],
            device_id={"fft": device_of(a)},
        )

    def in2(b, c, d):
        return pltpu.make_async_remote_copy(
            src_ref=send2.at[b, 0, pl.ds(0, piece), :],
            dst_ref=recv2.at[b, pl.ds(d * block + c * piece, piece), :],
            send_sem=ssend2.at[b, c, 0],
            recv_sem=srecv2.at[b, c, d],
            device_id={"fft": (me + 1) % peers},
        )

    def own1(b):
        return pltpu.make_async_copy(
            send1.at[b, pl.ds(me * block, block), :], recv1.at[b, mine], own1_sem.at[b]
        )

    def own2(b, c):
        return pltpu.make_async_copy(
            send2.at[b, mine, pl.ds(c * piece, piece), :],
            recv2.at[b, pl.ds(me * block + c * piece, piece), :],
            own2_sem.at[b, c],
        )

    index = lax.broadcasted_iota(jnp.int32, (quarter, NY), 0)

    def masked(b, gx):
        rows = []
        limit = extent[pl.ds(gx, 1), :]
        for half in range(2):
            height = index if half == 0 else quarter - index
            keep = height <= limit
            real = jnp.where(keep, waves[b, 0, half, gx], 0.0)
            imag = jnp.where(keep, waves[b, 1, half, gx], 0.0)
            rows.append(real + pltpu.roll(imag, NY // 2, 1))
        return jnp.concatenate(rows, axis=0)

    def to_planes(b):
        def step(i, c):
            values = [masked(b, 2 * i + j) for j in range(2)]
            both = jnp.concatenate(
                [jnp.concatenate([v, packed_i(v)], axis=0) for v in values], axis=1
            )
            high, low = split(both)
            planes = table_left(inv_z, high, low)
            for j in range(2):
                send1[b, pl.ds(2 * i + j, NZ, stride=gxl), :] = planes[:, j * NY : (j + 1) * NY]
            return c

        lax.fori_loop(0, gxl // 2, step, 0)

    def start1(b):
        own1(b).start()
        for c in range(chunks):
            def go(k, carry):
                out1(b, c, (me + k) % peers).start()
                return carry

            lax.fori_loop(1, peers, go, 0)

    for fetch in fetches:
        fetch.wait()

    for b in range(bands):
        @pl.when(is_active)
        def _():
            for where in loads:
                if where[0] == b:
                    load(wave, waves, wave_sem, *where).wait()
            to_planes(b)
            start1(b)

        if b == 0:
            lax.fori_loop(1, groups, vstart, 0)

            @pl.when(is_active)
            def _():
                for where in loads:
                    load(previous, prevs, prev_sem, *where).start()

    def real_space(b, i):
        rows = []
        for j in range(depth):
            z = i * depth + j
            for a in range(active):
                rows.append(recv1[b, a, pl.ds(pl.multiple_of(z * gxl, gxl), gxl), :])
        lines = table_right(jnp.concatenate(rows, axis=0), inv_y)
        back = []
        for j in range(depth):
            high, low = with_i(lines[j * kept_x : (j + 1) * kept_x])
            field = table_left(inv_x, high, low)
            v = vbuf[pl.ds(i * depth + j, NX, stride=zl), :]
            product = field * jnp.concatenate([v, v], axis=1)
            high, low = with_i(product)
            back.append(table_left(fwd_x, high, low))
        result = table_right(jnp.concatenate(back, axis=0), fwd_y)
        for j in range(depth):
            z = i * depth + j
            for a in range(active):
                first = j * kept_x + a * gxl
                send2[b, a, pl.ds(pl.multiple_of(z * gxl, gxl), gxl), :] = result[
                    first : first + gxl
                ]

    def vwait(k, c):
        vcopy(k).wait_recv()
        return c

    for b in range(bands):
        @pl.when(is_active)
        def _():
            own1(b).wait()

        if b == 0:
            vown.wait()

            lax.fori_loop(1, groups, vwait, 0)

        def chunk(c, carry):
            def wait1(a, inner):
                @pl.when(device_of(a) != me)
                def _():
                    in1(b, c, a).wait_recv()

                return inner

            lax.fori_loop(0, active, wait1, 0)
            real_space(b, c)

            def go2(k, inner):
                a = (mine + k) % active

                @pl.when(device_of(a) != me)
                def _():
                    out2(b, c, a).start()

                return inner

            lax.fori_loop(0, active, go2, 0)

            @pl.when(is_active)
            def _():
                own2(b, c).start()

            return carry

        lax.fori_loop(0, chunks, chunk, 0)

    shape = (quarter, NY)
    two_pi = 2.0 * math.pi
    lane = lax.broadcasted_iota(jnp.int32, shape, 1)
    sy = jnp.where(lane < NY // 2, lane, lane - NY)
    is_real = (lane < NY // 4) | (lane >= NY - NY // 4)
    ky = metric[1] * (two_pi * sy.astype(jnp.float32) / NY) ** 2
    factor = 2.0 / jnp.full(shape, halfwidth[0], jnp.float32)

    def finish(b, i, packed):
        gx = me * gxl + i
        sx = jnp.where(gx < NX // 2, gx, gx - NX)
        kx = metric[0] * (two_pi * jnp.full(shape, sx, jnp.int32).astype(jnp.float32) / NX) ** 2
        limit = extent[pl.ds(i, 1), :]
        for half in range(2):
            sz = index - half * quarter
            kz = metric[2] * (two_pi * sz.astype(jnp.float32) / NZ) ** 2
            kinetic = 0.5 * (kx + kz + ky)
            keep = (jnp.abs(sz) <= limit) & is_real
            value = packed[half * quarter : (half + 1) * quarter]
            values = (value, pltpu.roll(value, NY // 2, 1))
            for part in range(2):
                coeff = waves[b, part, half, i]
                next_value = factor * ((kinetic - center[0]) * coeff + values[part])
                compact[part, b, i, half] = jnp.where(
                    keep, next_value - prevs[b, part, half, i], 0.0
                )

    @pl.when(is_active)
    def _():
        for where in loads:
            load(previous, prevs, prev_sem, *where).wait()
        for b in range(bands):
            for c in range(chunks):
                def wait2(d, carry):
                    @pl.when(d != me)
                    def _():
                        in2(b, c, d).wait_recv()

                    return carry

                lax.fori_loop(0, peers, wait2, 0)
                own2(b, c).wait()

            def last(i, c):
                values = [recv2[b, pl.ds(2 * i + j, NZ, stride=gxl), :] for j in range(2)]
                both = jnp.concatenate(
                    [jnp.concatenate([v, packed_i(v)], axis=0) for v in values], axis=1
                )
                high, low = split(both)
                columns = table_left(fwd_z, high, low)
                for j in range(2):
                    finish(b, 2 * i + j, columns[:, j * NY : (j + 1) * NY])
                return c

            lax.fori_loop(0, gxl // 2, last, 0)
            for c in range(chunks):
                def sent1(k, carry):
                    out1(b, c, (me + k) % peers).wait_send()
                    return carry

                lax.fori_loop(1, peers, sent1, 0)

    @pl.when(jnp.logical_not(is_active))
    def _():
        compact[...] = jnp.zeros_like(compact)

    for b in range(bands):
        for c in range(chunks):
            def sent2(a, carry):
                @pl.when(device_of(a) != me)
                def _():
                    out2(b, c, a).wait_send()

                return carry

            lax.fori_loop(0, active, sent2, 0)

    def vsent(k, c):
        vcopy(k).wait_send()
        return c

    lax.fori_loop(1, groups, vsent, 0)


def place(compact, out, zeros, sem):
    _, bands, _, _, quarter, _ = compact.shape
    zeros[...] = jnp.zeros_like(zeros)
    copies = []
    for part in range(2):
        for b in range(bands):
            middle = out.at[part, b, :, pl.ds(quarter, NZ - 2 * quarter), :]
            copies.append((zeros, middle))
            for half in range(2):
                rows = out.at[part, b, :, pl.ds(half * (NZ - quarter), quarter), :]
                copies.append((compact.at[part, b, :, half], rows))
    copies = [pltpu.make_async_copy(*ends, sem.at[i]) for i, ends in enumerate(copies)]
    for copy in copies:
        copy.start()
    for copy in copies:
        copy.wait()


def fused(groups, peers, wave, previous, potential, column_extent, metric, center, halfwidth):
    _, bands, gxl = wave.shape[:3]
    quarter = NZ // 4
    active = peers // 2
    zl = NZ // peers
    block = zl * gxl
    chunks = zl // 4 if zl % 4 == 0 else zl
    f32 = jnp.float32
    vmem = pl.BlockSpec(memory_space=pltpu.VMEM)
    smem = pl.BlockSpec(memory_space=pltpu.SMEM)
    hbm = pl.BlockSpec(memory_space=pltpu.HBM)
    dma = pltpu.SemaphoreType.DMA
    flat = potential.reshape(potential.shape[0] * potential.shape[1], NY)
    tables_in = dft_tables()
    compact = pl.pallas_call(
        functools.partial(exchange, groups, peers),
        out_shape=jax.ShapeDtypeStruct((2, bands, gxl, 2, quarter, NY), f32),
        in_specs=[smem] * 3 + [hbm] * 3 + [vmem] + [hbm] * 6,
        out_specs=vmem,
        scratch_shapes=[pltpu.VMEM(t.shape, t.dtype) for t in tables_in] + [
            pltpu.VMEM((bands, 2, 2, gxl, quarter, NY), f32),
            pltpu.VMEM((bands, 2, 2, gxl, quarter, NY), f32),
            pltpu.VMEM((bands, NZ * gxl, NY), f32),
            pltpu.VMEM((bands, active, block, NY), f32),
            pltpu.VMEM((NX * zl, NY), f32),
            pltpu.VMEM((bands, active, block, NY), f32),
            pltpu.VMEM((bands, NZ * gxl, NY), f32),
            dma((6,)),
            dma((bands, 2, 2)),
            dma((bands, 2, 2)),
            dma((1,)),
            dma((bands,)),
            dma((bands, chunks)),
            dma((groups,)),
            dma((groups,)),
            dma((bands, chunks, peers)),
            dma((bands, chunks, active)),
            dma((bands, chunks, active)),
            dma((bands, chunks, peers)),
        ],
        compiler_params=pltpu.CompilerParams(
            collective_id=0, has_side_effects=True, vmem_limit_bytes=67043328 - 4 * wave.size // 2
        ),
        name="exchange",
    )(metric, center, halfwidth, wave, previous, flat, column_extent, *tables_in)
    return pl.pallas_call(
        place,
        out_shape=jax.ShapeDtypeStruct(wave.shape, f32),
        in_specs=[pl.BlockSpec(memory_space=pl.ANY)],
        out_specs=hbm,
        scratch_shapes=[pltpu.VMEM((gxl, NZ - 2 * quarter, NY), f32), dma((6 * bands,))],
        compiler_params=pltpu.CompilerParams(vmem_limit_bytes=8 * 2**20),
        name="place",
    )(compact)


def solution(mesh):
    in_specs = (
        P(None, "band", "fft", None, None),
        P(None, "band", "fft", None, None),
        P("band", "fft", None),
        P("fft", None),
        P(),
        P(),
        P(),
    )
    out_specs = P(None, "band", "fft", None, None)
    groups, peers = mesh.shape["band"], mesh.shape["fft"]
    body = local
    if peers % 4 == 0 and (NX // peers) % 8 == 0:
        body = functools.partial(fused, groups, peers)
    return jax.shard_map(body, mesh=mesh, in_specs=in_specs, out_specs=out_specs, check_vma=False)
```
